32 devices in a mesh: rep: 2 (over x), shard: 16 (over z, y, core).
Axes of the slice: x: 2, y: 2, z: 4, core: 2. Of those that a mesh axis runs over, the one named last changes fastest.
Arguments:
- features: float32 [16384, 256], P(('rep', 'shard')), may hold values from -6 to 6
- seed_self: float32 [4096, 256], P(('rep', 'shard')), may hold values from -6 to 6
- hub_ids: int32 [4096], P(('rep', 'shard')), may hold values from 0 to 511
- requests: int32 [512, 32], P(('rep', 'shard')), may hold values from 0 to 511
- counts: int32 [512], P(('rep', 'shard')), may hold values from 1 to 32, as said below
- neighbors: int32 [4096, 15], P(('rep', 'shard')), may hold values from 0 to 767
- weight: float32 [256, 256], replicated, may hold values from -1 to 1
- out_bias: float32 [256], replicated, may hold values from -4 to 4
Outputs:
- embedded: float32 [4096, 256], P(('rep', 'shard'))
The draws below stay inside these ranges and needn't reach their ends.
Inputs may be any that keep to these rules, and one draw needn't show every extreme that they name: `hub_ids`: offsets into the block of features of the same device. `requests`: row d of a device's lists holds offsets into the block of features of the device at shard index d with the same rep index; empty slots hold offsets too. counts[r, s, d] slots of the list from shard index s to shard index d are live, the first ones; for every rep index some destination has 32 live slots from every source. `neighbors`: A code below 256 names a row of the device's hub cache; a code 256 + d * 32 + c names slot c of the device's list to shard index d, and counts only where that slot is live.
All inputs are finite; a program needn't handle non-finite values.
Results may differ from the reference program's by a relative error of at most 0.0003.
Values sent between devices are 32-bit elements; how exact they have to be, the bound alone decides.
No kernel may reach another device: no remote copies, remote signals or barrier semaphores. Data moves between devices by JAX's collectives and lax.ppermute only.
A program may use at most 64 MiB of HBM per device.

```python
import jax
import jax.numpy as jnp
from jax import lax

F = 256
FANOUT = 15
CAP = 32
ROWS_DEV = 512
SEEDS_DEV = 128
HUB_DEV = 128
HUBS = 256
SLOTS_DEV = 512
CODES = 768
NODES = 16384
SEEDS = 4096
HUB_SLOTS = 4096
REQ_ROWS = 512
N_REP = 2
N_SHARD = 16


def draw_counts(key, part):
    k_base, k_owner = jax.random.split(jax.random.fold_in(key, 11), 2)
    base_fill = jax.random.randint(k_base, (N_REP, N_SHARD, N_SHARD), CAP // 4, CAP + 1)
    full_owner = jax.random.randint(k_owner, (N_REP, 1, 1), 0, N_SHARD)
    owner_index = lax.broadcasted_iota(jnp.int32, (N_REP, N_SHARD, N_SHARD), 2)
    result = jnp.where(owner_index == full_owner, CAP, base_fill)
    return result.reshape(-1).astype(jnp.int32)


def plant(entries, rng, low, top_value):
    longest = entries.shape.index(max(entries.shape))
    spots = []
    for shift in (0, 1):
        where = [jax.random.randint(jax.random.fold_in(rng, axis), (), 0, length) for axis, length in enumerate(entries.shape)]
        where[longest] = (where[longest] + shift) % entries.shape[longest]
        spots.append(tuple(where))
    return entries.at[spots[0]].set(low).at[spots[1]].set(top_value)


def steps_of(stream_key, extent, shards, low, largest):
    gain = 1.0
    for position, parts in shards:
        steps = jax.random.uniform(jax.random.fold_in(jax.random.fold_in(stream_key, 6), position), (parts,), jnp.float32, low / len(shards), largest / len(shards))
        gain = gain * jnp.repeat(jnp.exp(steps), extent[position] // parts).reshape((-1,) + (1,) * (len(extent) - 1 - position))
    return gain


def bell_draw(rng, extent, deviation, bound, cuts=(), kind=jnp.bfloat16):
    level = steps_of(rng, extent, cuts, -0.22, 0.18) if cuts else 1.0
    values = jax.random.normal(rng, extent, jnp.float32) * deviation * level
    return jnp.minimum(jnp.maximum(values, -bound), bound).astype(kind)


def setup_inputs(seed: int = 0) -> dict:
    seeds = jax.random.split(jax.random.key(seed), 9)
    features = bell_draw(seeds[0], (NODES, F), 1.0, 6.0, ((0, 32),), jnp.float32)
    seed_self = bell_draw(seeds[1], (SEEDS, F), 1.0, 6.0, ((0, 32),), jnp.float32)
    hub_ids = plant(jax.random.randint(seeds[2], (HUB_SLOTS,), 0, ROWS_DEV), jax.random.fold_in(seeds[2], 1), 0, ROWS_DEV - 1).astype(jnp.int32)
    requests = plant(jax.random.randint(seeds[3], (REQ_ROWS, CAP), 0, ROWS_DEV), jax.random.fold_in(seeds[3], 1), 0, ROWS_DEV - 1).astype(jnp.int32)
    counts = draw_counts(jax.random.fold_in(seeds[8], 71), 0)
    neighbors = plant(jax.random.randint(seeds[5], (SEEDS, FANOUT), 0, CODES), jax.random.fold_in(seeds[5], 1), 0, CODES - 1).astype(jnp.int32)
    weight = bell_draw(seeds[6], (F, F), (F // 8) ** -0.5, 1.0, (), jnp.float32)
    out_bias = bell_draw(seeds[7], (F,), 1.0, 4.0, (), jnp.float32)
    return dict(features=features, seed_self=seed_self, hub_ids=hub_ids, requests=requests, counts=counts, neighbors=neighbors, weight=weight, out_bias=out_bias)


def reference(features, seed_self, hub_ids, requests, counts, neighbors, weight, out_bias):
    blocks = features.reshape(N_REP, N_SHARD, ROWS_DEV, F)
    hub_index = hub_ids.reshape(N_REP, N_SHARD, HUB_DEV)
    request_index = requests.reshape(N_REP, N_SHARD, N_SHARD, CAP)
    fill_counts = counts.reshape(N_REP, N_SHARD, N_SHARD)
    neighbor_codes = neighbors.reshape(N_REP * N_SHARD, SEEDS_DEV, FANOUT)
    own_rows = seed_self.reshape(N_REP * N_SHARD, SEEDS_DEV, F)
    rep_iota = jnp.arange(N_REP, dtype=jnp.int32)[:, None]
    shard_iota = jnp.arange(N_SHARD, dtype=jnp.int32)[:, None]
    slot_iota = jnp.arange(CAP, dtype=jnp.int32)[None, :]

    def per_device(device_index):
        rep_pos = device_index // N_SHARD
        shard_pos = device_index % N_SHARD
        hub_cache = blocks[rep_iota, shard_pos, hub_index[:, shard_pos]].reshape(HUBS, F)
        fetched = blocks[rep_pos, shard_iota, request_index[rep_pos, shard_pos]].reshape(SLOTS_DEV, F)
        source = jnp.concatenate([hub_cache, fetched], axis=0)
        slot_live = (slot_iota < fill_counts[rep_pos, shard_pos][:, None]).astype(jnp.float32)
        live = jnp.concatenate([jnp.ones((HUBS,), jnp.float32), slot_live.reshape(SLOTS_DEV)])
        codes = neighbor_codes[device_index]
        picked = source[codes]
        weights = live[codes]
        total = own_rows[device_index] + jnp.sum(picked * weights[:, :, None], axis=1)
        taken = 1.0 + jnp.sum(weights, axis=1)
        mean_rows = total / taken[:, None]
        product = jnp.dot(mean_rows, weight, precision=lax.Precision.HIGHEST, preferred_element_type=jnp.float32)
        return jnp.maximum(product + out_bias, 0.0)

    result = lax.map(per_device, jnp.arange(N_REP * N_SHARD, dtype=jnp.int32))
    return result.reshape(SEEDS, F)
```

```python
import jax
import jax.numpy as jnp
from jax import lax
from jax.sharding import PartitionSpec as P


def dot(a, b):
    return jnp.dot(a, b, precision=lax.Precision.HIGH, preferred_element_type=jnp.float32)


def tally_of(codes, code_row):
    tally = jnp.zeros((codes.shape[0], code_row.shape[1]), jnp.float32)
    for column in range(codes.shape[1]):
        tally = tally + (codes[:, column : column + 1] == code_row).astype(jnp.float32)
    return tally


def local(features, seed_self, hub_ids, requests, counts, neighbors, weight, out_bias):
    shard_count, capacity = requests.shape
    feat_width = features.shape[1]
    reps = lax.axis_size("rep")
    rep = lax.axis_index("rep")
    hubs = hub_ids.shape[0]
    hub_total = hubs * reps

    asked = lax.all_to_all(requests, "shard", split_axis=0, concat_axis=0, tiled=True)

    own = features.at[hub_ids].get(mode="promise_in_bounds")
    blocks = [own]
    offsets = [rep * hubs]
    for k in range(1, reps):
        blocks.append(lax.ppermute(own, "rep", [(i, (i + k) % reps) for i in range(reps)]))
        offsets.append(((rep - k) % reps) * hubs)
    hub_iota = lax.broadcasted_iota(jnp.int32, (1, hubs), 1)
    hub_codes = jnp.concatenate([hub_iota + o for o in offsets], axis=1)

    slot = lax.broadcasted_iota(jnp.int32, (shard_count, capacity), 1)
    flat = lax.broadcasted_iota(jnp.int32, (shard_count, capacity), 0) * capacity + slot
    slot_codes = jnp.where(slot < counts[:, None], flat + hub_total, -1).reshape(1, -1)
    hub_tally = tally_of(neighbors, hub_codes)
    slot_tally = tally_of(neighbors, slot_codes)
    taken = 1.0 + jnp.sum(hub_tally, axis=1) + jnp.sum(slot_tally, axis=1)
    hub_tally, slot_tally, taken, asked = lax.optimization_barrier(
        (hub_tally, slot_tally, taken, asked)
    )

    looked = features.at[asked].get(mode="promise_in_bounds")
    fetched = lax.all_to_all(looked, "shard", split_axis=0, concat_axis=0, tiled=True)
    hub_rows = jnp.concatenate(blocks, axis=0)
    base = seed_self + dot(hub_tally, hub_rows)
    total = base + dot(slot_tally, fetched.reshape(-1, feat_width))
    mean_rows = total / taken[:, None]
    return jnp.maximum(dot(mean_rows, weight) + out_bias, 0.0)


def solution(mesh):
    both = P(("rep", "shard"))
    return jax.shard_map(
        local,
        mesh=mesh,
        in_specs=(both, both, both, both, both, both, P(), P()),
        out_specs=both,
        check_vma=False,
    )
```

```python
import jax
import jax.numpy as jnp
from jax import lax
from jax.experimental import pallas as pl
from jax.experimental.pallas import tpu as pltpu
from jax.sharding import PartitionSpec as P


F32 = jnp.float32
BF16 = jnp.bfloat16
VMEM = pl.BlockSpec(memory_space=pltpu.VMEM)
SMEM = pl.BlockSpec(memory_space=pltpu.SMEM)


def mm(a, b):
    return jnp.dot(a, b, preferred_element_type=F32)


def split(x):
    hi = x.astype(BF16)
    return hi, (x - hi.astype(F32)).astype(BF16)


def prepare(tables, hub_blocks, neighbors, hub_codes, slot_codes, seed_self):
    n_tab, n_hub = len(tables), len(hub_blocks)
    rows, width = tables[0].shape
    seeds = seed_self.shape[0]

    def body(*refs):
        tabs, hubs = refs[:n_tab], refs[n_tab : n_tab + n_hub]
        nbr, hcode, scode, own = refs[n_tab + n_hub : n_tab + n_hub + 4]
        hi_ref, lo_ref, base_ref, tally_ref, taken_ref = refs[n_tab + n_hub + 4 :]
        for p in range(n_tab):
            hi, lo = split(tabs[p][...])
            hi_ref[pl.ds(p * rows, rows), :] = hi
            lo_ref[pl.ds(p * rows, rows), :] = lo

        def tally_of(code_row):
            tally = jnp.zeros((seeds, code_row.shape[1]), F32)
            for j in range(nbr.shape[1]):
                tally = tally + jnp.where(nbr[:, j : j + 1] == code_row, 1.0, 0.0)
            return tally

        hub_tally = tally_of(hcode[...])
        slot_tally = tally_of(scode[...])
        taken_ref[...] = (
            1.0
            + jnp.sum(hub_tally, axis=1, keepdims=True)
            + jnp.sum(slot_tally, axis=1, keepdims=True)
        )
        tally_ref[...] = slot_tally.astype(BF16)
        hi, lo = split(jnp.concatenate([h[...] for h in hubs], axis=0))
        ht = hub_tally.astype(BF16)
        base_ref[...] = own[...] + (mm(ht, hi) + mm(ht, lo))

    sds = jax.ShapeDtypeStruct
    return pl.pallas_call(
        body,
        in_specs=[VMEM] * (n_tab + n_hub + 4),
        out_specs=[VMEM] * 5,
        out_shape=[
            sds((n_tab * rows, width), BF16),
            sds((n_tab * rows, width), BF16),
            sds((seeds, width), F32),
            sds((seeds, slot_codes.shape[1]), BF16),
            sds((seeds, 1), F32),
        ],
        name="prepare",
    )(*tables, *hub_blocks, neighbors, hub_codes, slot_codes, seed_self)


def look_up(lists, asked, hi, lo, n_tab, groups):
    cap = asked.shape[1]
    rows, width = hi.shape[0] // n_tab, hi.shape[1]

    def body(list_ref, asked_ref, hi_ref, lo_ref, *outs):
        for p in range(n_tab):
            ids = jnp.concatenate(
                [asked_ref[pl.ds(list_ref[p, k], 1), :] for k in range(groups)], axis=1
            )
            iota = lax.broadcasted_iota(jnp.int32, (rows, groups * cap), 0)
            pick = jnp.where(iota == ids, 1.0, 0.0).astype(BF16)
            dims = (((0,), (0,)), ((), ()))
            got = lax.dot_general(
                pick, hi_ref[pl.ds(p * rows, rows), :], dims, preferred_element_type=F32
            ) + lax.dot_general(
                pick, lo_ref[pl.ds(p * rows, rows), :], dims, preferred_element_type=F32
            )
            start = (list_ref[p, 0] % n_tab) * cap
            for k in range(groups):
                outs[k][pl.ds(pl.multiple_of(start, 8), cap), :] = got[k * cap : (k + 1) * cap]

    return pl.pallas_call(
        body,
        in_specs=[SMEM, VMEM, VMEM, VMEM],
        out_specs=[VMEM] * groups,
        out_shape=[jax.ShapeDtypeStruct((n_tab * cap, width), F32)] * groups,
        name="look_up",
    )(lists, asked, hi, lo)


def finish(base, tally, taken, weight, bias, blocks):
    def body(base_ref, tally_ref, taken_ref, w_ref, b_ref, *refs):
        wh, wl = split(w_ref[...])
        hi, lo = split(jnp.concatenate([r[...] for r in refs[:-1]], axis=0))
        t = tally_ref[...]
        total = base_ref[...] + (mm(t, hi) + mm(t, lo))
        mh, ml = split(total / taken_ref[...])
        product = mm(mh, wh) + (mm(mh, wl) + mm(ml, wh))
        refs[-1][...] = jnp.maximum(product + b_ref[...], 0.0)

    return pl.pallas_call(
        body,
        in_specs=[VMEM] * (5 + len(blocks)),
        out_specs=VMEM,
        out_shape=jax.ShapeDtypeStruct(base.shape, F32),
        name="finish",
    )(base, tally, taken, weight, bias, *blocks)


def local(features, seed_self, hub_ids, requests, counts, neighbors, weight, out_bias):
    shard_count, capacity = requests.shape
    reps = lax.axis_size("rep")
    rep = lax.axis_index("rep")
    hubs = hub_ids.shape[0]
    hub_total = hubs * reps
    n_tab = 2 if shard_count % 2 == 0 else 1
    groups = shard_count // n_tab
    me = lax.axis_index("shard")
    group, lane = me // n_tab, me % n_tab
    xor = groups & (groups - 1) == 0

    def partner(g, k):
        return g ^ k if xor else (g + k) % groups

    def source(g, k):
        return g ^ k if xor else (g - k) % groups

    asked = lax.all_to_all(
        requests,
        "shard",
        split_axis=0,
        concat_axis=0,
        axis_index_groups=[[g * n_tab + p for g in range(groups)] for p in range(n_tab)],
        tiled=True,
    )
    tables = [features]
    if n_tab == 2:
        tables.append(lax.ppermute(features, "shard", [(i, i ^ 1) for i in range(shard_count)]))

    own = features.at[hub_ids].get(mode="promise_in_bounds")
    hub_blocks = [own]
    offsets = [rep * hubs]
    for k in range(1, reps):
        hub_blocks.append(lax.ppermute(own, "rep", [(i, (i + k) % reps) for i in range(reps)]))
        offsets.append(((rep - k) % reps) * hubs)
    hub_iota = lax.broadcasted_iota(jnp.int32, (1, hubs), 1)
    hub_codes = jnp.concatenate([hub_iota + o for o in offsets], axis=1)

    slot = lax.broadcasted_iota(jnp.int32, (shard_count, capacity), 1)
    flat = lax.broadcasted_iota(jnp.int32, (shard_count, capacity), 0) * capacity + slot
    slot_codes = jnp.where(slot < counts[:, None], flat + hub_total, -1)
    slot_codes = slot_codes.reshape(groups, n_tab * capacity)
    stages = jnp.arange(groups, dtype=jnp.int32)
    slot_codes = slot_codes.at[source(group, stages)].get(mode="promise_in_bounds").reshape(1, -1)

    hi, lo, base, tally, taken = prepare(
        tables, hub_blocks, neighbors, hub_codes, slot_codes, seed_self
    )
    lists = jnp.stack(
        [partner(group, stages) * n_tab + (lane ^ p) for p in range(n_tab)], axis=0
    ).astype(jnp.int32)
    blocks = list(look_up(lists, asked, hi, lo, n_tab, groups))
    for k in range(1, groups):
        blocks[k] = lax.ppermute(
            blocks[k],
            "shard",
            [(i, partner(i // n_tab, k) * n_tab + i % n_tab) for i in range(shard_count)],
        )
    return finish(base, tally, taken, weight, out_bias.reshape(1, -1), blocks)


def solution(mesh):
    both = P(("rep", "shard"))
    return jax.shard_map(
        local,
        mesh=mesh,
        in_specs=(both, both, both, both, both, both, P(), P()),
        out_specs=both,
        check_vma=False,
    )
```

```python
import jax
import jax.numpy as jnp
from jax import lax
from jax.sharding import PartitionSpec as P


def dot(a, b):
    return jnp.dot(a, b, precision=lax.Precision.HIGH, preferred_element_type=jnp.float32)


def tally_of(codes, code_row):
    tally = jnp.zeros((codes.shape[0], code_row.shape[1]), jnp.float32)
    for column in range(codes.shape[1]):
        tally = tally + (codes[:, column : column + 1] == code_row).astype(jnp.float32)
    return tally


def local(features, seed_self, hub_ids, requests, counts, neighbors, weight, out_bias):
    shard_count, capacity = requests.shape
    feat_width = features.shape[1]
    reps = lax.axis_size("rep")
    rep = lax.axis_index("rep")
    hubs = hub_ids.shape[0]
    hub_total = hubs * reps

    asked = lax.all_to_all(requests, "shard", split_axis=0, concat_axis=0, tiled=True)

    own = features.at[hub_ids].get(mode="promise_in_bounds")
    blocks = [own]
    offsets = [rep * hubs]
    for k in range(1, reps):
        blocks.append(lax.ppermute(own, "rep", [(i, (i + k) % reps) for i in range(reps)]))
        offsets.append(((rep - k) % reps) * hubs)
    hub_iota = lax.broadcasted_iota(jnp.int32, (1, hubs), 1)
    hub_codes = jnp.concatenate([hub_iota + o for o in offsets], axis=1)

    slot = lax.broadcasted_iota(jnp.int32, (shard_count, capacity), 1)
    flat = lax.broadcasted_iota(jnp.int32, (shard_count, capacity), 0) * capacity + slot
    slot_codes = jnp.where(slot < counts[:, None], flat + hub_total, -1).reshape(1, -1)
    hub_tally = tally_of(neighbors, hub_codes)
    slot_tally = tally_of(neighbors, slot_codes)
    taken = 1.0 + jnp.sum(hub_tally, axis=1) + jnp.sum(slot_tally, axis=1)
    hub_tally, slot_tally, taken, asked = lax.optimization_barrier(
        (hub_tally, slot_tally, taken, asked)
    )

    row_iota = lax.broadcasted_iota(jnp.int32, (1, 1, features.shape[0]), 2)
    picks = (asked[:, :, None] == row_iota).astype(jnp.float32)
    looked = lax.dot_general(
        picks,
        features,
        (((2,), (0,)), ((), ())),
        precision=lax.Precision.HIGH,
        preferred_element_type=jnp.float32,
    )
    fetched = lax.all_to_all(looked, "shard", split_axis=0, concat_axis=0, tiled=True)
    hub_rows = jnp.concatenate(blocks, axis=0)
    base = seed_self + dot(hub_tally, hub_rows)
    total = base + dot(slot_tally, fetched.reshape(-1, feat_width))
    mean_rows = total / taken[:, None]
    return jnp.maximum(dot(mean_rows, weight) + out_bias, 0.0)


def solution(mesh):
    both = P(("rep", "shard"))
    return jax.shard_map(
        local,
        mesh=mesh,
        in_specs=(both, both, both, both, both, both, P(), P()),
        out_specs=both,
        check_vma=False,
    )
```
